32 devices in a mesh: gx: 4 (over y, x), gz: 8 (over z, core).
Axes of the slice: x: 2, y: 2, z: 4, core: 2. Of those that a mesh axis runs over, the one named last changes fastest.
Arguments:
- divergence: float32 [256, 128, 512], P('gx', 'gz'), may hold values from -18 to 18
- level_set: float32 [256, 128, 512], P('gx', 'gz'), may hold values from -2 to 2, as said below
- tile_ids: int32 [4, 8192], P('gx', 'gz'), may hold values from -1 to 1023, as said below
Outputs:
- pressure: float32 [256, 128, 512], P('gx', 'gz')
- residual: float32 [256, 128, 512], P('gx', 'gz')
The draws below stay inside these ranges and needn't reach their ends.
Inputs may be any that keep to these rules, and one draw needn't show every extreme that they name: `level_set`: every entry lies at least 0.05 away from zero. `tile_ids`: each device's part lists distinct tile numbers of its own block, below 1024, in increasing order, followed by -1 entries; some device lists all 1024 and some device lists none.
All inputs are finite; a program needn't handle non-finite values.
Results may differ from the reference program's by a relative error of at most 0.0003.
Values sent between devices are 32-bit elements; how exact they have to be, the bound alone decides.
No kernel may reach another device: no remote copies, remote signals or barrier semaphores. Data moves between devices by JAX's collectives and lax.ppermute only.
A program may use at most 128 MiB of HBM per device.

```python
import math
import jax
import jax.numpy as jnp
from jax import lax

CX = 64
CZ = 16
NY = 512
ITERS = 2
TILE = 8
NX = 256
NZ = 128
TILES_DEV = 1024
SLOTS = 1024
N_GX = 4
N_GZ = 8


def surface_height(key):
    lowest = 35 * NZ // 100
    highest = 75 * NZ // 100
    return jax.random.randint(jax.random.fold_in(key, 12), (NX, NY), lowest, highest).astype(jnp.int32)


def draw_level_set(key, part):
    shape = (NX, NZ, NY)
    mag_key = jax.random.fold_in(key, 11)
    flip_key = jax.random.fold_in(key, 13)
    magnitude = jnp.exp(jax.random.uniform(mag_key, shape, jnp.float32, math.log(0.05), math.log(2.0)))
    magnitude = jnp.clip(magnitude, 0.05, 2.0)
    height = surface_height(key)[:, None, :]
    levels = lax.broadcasted_iota(jnp.int32, (1, NZ, 1), 1)
    bulk = levels < height
    nearby = jnp.abs(levels - height) <= 3
    flipped = jnp.logical_and(nearby, jax.random.randint(flip_key, shape, 0, 10) == 0)
    inside = jnp.logical_xor(bulk, flipped)
    return jnp.where(inside, -magnitude, magnitude)


def draw_tile_ids(key, part):
    devices = N_GX * N_GZ
    counts = jax.random.randint(jax.random.fold_in(key, 21), (devices,), 0, TILES_DEV + 1).astype(jnp.int32)
    device_order = jax.random.permutation(jax.random.fold_in(key, 22), devices).astype(jnp.int32)
    counts = jnp.where(device_order == 0, TILES_DEV, jnp.where(device_order == 1, 0, counts)).astype(jnp.int32)
    device_keys = jax.random.split(jax.random.fold_in(key, 23), devices)
    ranking = jax.vmap(lambda single: jax.random.permutation(single, TILES_DEV))(device_keys).astype(jnp.int32)
    chosen = ranking < counts[:, None]
    numbers = lax.broadcasted_iota(jnp.int32, (devices, TILES_DEV), 1)
    scores = jnp.where(chosen, numbers, numbers + TILES_DEV).astype(jnp.int32)
    ordered = jnp.sort(scores, axis=1)
    listed = jnp.where(ordered < TILES_DEV, ordered, -1).astype(jnp.int32)
    return listed.reshape(N_GX, N_GZ * SLOTS).astype(jnp.int32)


def block_scale(stream_key, shape, cuts, least, top_value):
    level, own = 1.0, jax.random.fold_in(stream_key, 6)
    for position, parts in cuts:
        draws = jnp.exp(jax.random.uniform(jax.random.fold_in(own, position), (parts,), jnp.float32, least / len(cuts), top_value / len(cuts)))
        level = level * jnp.repeat(draws, shape[position] // parts).reshape([-1 if axis == position else 1 for axis in range(len(shape))])
    return level


def centred(rng, extent, deviation, most, cuts=(), held_as=jnp.bfloat16):
    drawn = jax.random.normal(rng, extent, jnp.float32) * deviation
    if len(cuts) > 0:
        drawn = block_scale(rng, extent, cuts, -0.22, 0.18) * drawn
    return jnp.clip(drawn, min=-most, max=most).astype(held_as)


def setup_inputs(seed: int = 0) -> dict:
    key_of = jax.random.split(jax.random.key(seed), 4)
    divergence = centred(key_of[0], (NX, NZ, NY), 3.0, 18.0, ((0, 4), (1, 8)), jnp.float32)
    level_set = draw_level_set(jax.random.fold_in(key_of[3], 71), 0)
    tile_ids = draw_tile_ids(jax.random.fold_in(key_of[3], 71), 0)
    return dict(divergence=divergence, level_set=level_set, tile_ids=tile_ids)


damping = 2.0 / 3.0
ratio_cap = 20.0


def neighbours(values):
    padded = jnp.pad(values, 1)
    return [padded[2:, 1:-1, 1:-1], padded[:-2, 1:-1, 1:-1], padded[1:-1, 2:, 1:-1], padded[1:-1, :-2, 1:-1], padded[1:-1, 1:-1, 2:], padded[1:-1, 1:-1, :-2]]


def summed(pieces):
    result = pieces[0] + pieces[1]
    for addend in pieces[2:]:
        result = result + addend
    return result


def diagonal_of(distance, fluid_cells):
    safe_dist = jnp.where(distance > 0, distance, 1.0)
    dist_near = neighbours(distance)
    fluid_near = neighbours(fluid_cells)
    term_list = [jnp.where(fluid_side > 0, 1.0, jnp.minimum((distance + dist_side) / safe_dist, ratio_cap)) for dist_side, fluid_side in zip(dist_near, fluid_near)]
    return jnp.where(fluid_cells > 0, summed(term_list), 1.0)


def operate(values, diagonal, fluid_cells):
    return fluid_cells * (diagonal * values - summed(neighbours(values)))


def smooth(residual, diagonal, fluid_cells, scale):
    first_pass = scale * residual
    second_pass = first_pass + scale * (residual - operate(first_pass, diagonal, fluid_cells))
    return second_pass, operate(second_pass, diagonal, fluid_cells)


def reference(divergence, level_set, tile_ids):
    listed = tile_ids.reshape(N_GX, N_GZ, SLOTS).astype(jnp.int32)
    device = lax.broadcasted_iota(jnp.int32, (N_GX, N_GZ, SLOTS), 0) * N_GZ + lax.broadcasted_iota(jnp.int32, (N_GX, N_GZ, SLOTS), 1)
    count_all = N_GX * N_GZ * TILES_DEV
    flat_ids = jnp.where(listed >= 0, device * TILES_DEV + listed, count_all).astype(jnp.int32)
    table = jnp.zeros((count_all + 1,), jnp.float32).at[flat_ids.reshape(-1)].set(1.0)[:count_all]
    table = table.reshape(N_GX, N_GZ, CX // TILE, CZ // TILE, NY // TILE).transpose(0, 2, 1, 3, 4)
    table = table.reshape(NX // TILE, NZ // TILE, NY // TILE)
    active = jnp.broadcast_to(table[:, None, :, None, :, None], (NX // TILE, TILE, NZ // TILE, TILE, NY // TILE, TILE)).reshape(NX, NZ, NY)
    fluid_cells = jnp.where(level_set < 0, active, 0.0)
    distance = jnp.abs(level_set)
    diagonal = diagonal_of(distance, fluid_cells)
    scale = damping / diagonal
    pressure = jnp.zeros_like(divergence)
    residual = fluid_cells * divergence
    smoothed, precond_image = smooth(residual, diagonal, fluid_cells, scale)
    gamma_now = jnp.sum(residual * smoothed)
    direction = smoothed
    operated = precond_image
    for iteration in range(ITERS):
        alpha_now = gamma_now / jnp.sum(direction * operated)
        pressure = pressure + alpha_now * direction
        residual = residual - alpha_now * operated
        if iteration + 1 < ITERS:
            smoothed, precond_image = smooth(residual, diagonal, fluid_cells, scale)
            gamma_next = jnp.sum(residual * smoothed)
            beta_now = gamma_next / gamma_now
            direction = smoothed + beta_now * direction
            operated = precond_image + beta_now * operated
            gamma_now = gamma_next
    return pressure, residual
```

```python
import functools

import jax
import jax.numpy as jnp
from jax import lax
from jax.experimental import pallas as pl
from jax.experimental.pallas import tpu as pltpu
from jax.sharding import PartitionSpec as P

TILE = 8
LANES = 128
HALO = 4
ITERS = 2
damping = 2.0 / 3.0
ratio_cap = 20.0
f32 = jnp.float32

VMEM_SPEC = pl.BlockSpec(memory_space=pltpu.VMEM)


def rows_of(shape):
    return lax.broadcasted_iota(jnp.int32, shape, 0)


def swap_halves(tile):
    return pltpu.roll(tile, HALO, 0)


def active_rows(ids_ref, tiles_x, tiles_z, tiles_y):
    ids = ids_ref[0:1, :]
    size_y = tiles_y * TILE
    slots = ids.shape[1]
    column = lax.div(lax.broadcasted_iota(jnp.int32, (size_y, slots), 0), TILE)
    along_y = (column == lax.rem(ids, tiles_y)).astype(f32)
    first = lax.broadcasted_iota(jnp.int32, (tiles_x, slots), 0) * (tiles_z * tiles_y)
    layers = []
    for layer in range(tiles_z):
        low = first + layer * tiles_y
        mine = jnp.logical_and(ids >= low, ids < low + tiles_y).astype(f32)
        layers.append(
            lax.dot_general(mine, along_y, (((1,), (1,)), ((), ())), preferred_element_type=f32)
        )
    return layers


def pack_x_kernel(dims, ids_hbm, ls_ref, div_ref, up_ref, down_ref, act_ref, buf, ids_ref, sems):
    size_x, size_z, size_y = dims
    deep = HALO + 1
    ids_copy = pltpu.make_async_copy(ids_hbm, ids_ref, sems.at[4])
    ids_copy.start()
    copies = [
        pltpu.make_async_copy(ls_ref.at[pl.ds(size_x - deep, deep)], buf.at[pl.ds(0, deep)], sems.at[0]),
        pltpu.make_async_copy(div_ref.at[pl.ds(size_x - HALO, HALO)], buf.at[pl.ds(deep, HALO)], sems.at[1]),
        pltpu.make_async_copy(ls_ref.at[pl.ds(0, deep)], buf.at[pl.ds(deep + HALO, deep)], sems.at[2]),
        pltpu.make_async_copy(div_ref.at[pl.ds(0, HALO)], buf.at[pl.ds(2 * deep + HALO, HALO)], sems.at[3]),
    ]
    for copy in copies:
        copy.start()
    tiles_z = size_z // TILE
    ids_copy.wait()
    layers = active_rows(ids_ref, size_x // TILE, tiles_z, size_y // TILE)
    flags = (deep + HALO) * size_z
    for layer in range(tiles_z):
        act_ref[layer] = layers[layer]
        up_ref[flags + layer : flags + layer + 1] = layers[layer][size_x // TILE - 1 :]
        down_ref[flags + layer : flags + layer + 1] = layers[layer][:1]
    for copy in copies:
        copy.wait()
    for plane in range(deep + HALO):
        up_ref[plane * size_z : (plane + 1) * size_z] = buf[plane]
        down_ref[plane * size_z : (plane + 1) * size_z] = buf[deep + HALO + plane]


def z_messages(low_ls, high_ls, low_div, high_div):
    first = rows_of(low_ls.shape) < HALO
    up = jnp.where(first, swap_halves(high_div), high_ls)
    down = jnp.where(first, low_ls, swap_halves(low_div))
    return up, down


def pack_z_kernel(dims, planes, ls_ref, div_ref, act_ref, up_ref, down_ref, flat_up, flat_down):
    size_x, size_z, size_y = dims
    step = pl.program_id(0)
    for p in range(planes):
        low_ls = ls_ref[p, 0:TILE]
        high_ls = ls_ref[p, size_z - TILE : size_z]
        up, down = z_messages(low_ls, high_ls, div_ref[p, 0:TILE], div_ref[p, size_z - TILE : size_z])
        row = pl.multiple_of((step * planes + p) * TILE, TILE)
        up_ref[pl.ds(row, TILE)] = up
        down_ref[pl.ds(row, TILE)] = down
        flat_up[p : p + 1] = high_ls[TILE - HALO - 1 : TILE - HALO]
        flat_down[p : p + 1] = low_ls[HALO : HALO + 1]
    row = pl.multiple_of(size_x * TILE + step * planes, planes)
    up_ref[pl.ds(row, planes)] = flat_up[...]
    down_ref[pl.ds(row, planes)] = flat_down[...]
    flags = size_x * (TILE + 1)
    tiles_x = size_x // TILE

    @pl.when(step == 0)
    def _():
        up_ref[flags : flags + tiles_x] = act_ref[size_z // TILE - 1]
        down_ref[flags : flags + tiles_x] = act_ref[0]


def pack_corner_kernel(dims, low_ref, high_ref, up_ref, down_ref):
    size_x, size_z, size_y = dims
    deep = HALO + 1
    fields = deep * size_z
    flags = (deep + HALO) * size_z
    for side, ref in ((0, low_ref), (1, high_ref)):
        for p in range(HALO):
            ls_row = (p + 1 - side) * size_z
            div_row = fields + p * size_z
            up, down = z_messages(
                ref[ls_row : ls_row + TILE],
                ref[ls_row + size_z - TILE : ls_row + size_z],
                ref[div_row : div_row + TILE],
                ref[div_row + size_z - TILE : div_row + size_z],
            )
            row = (side * HALO + p) * TILE
            up_ref[row : row + TILE] = up
            down_ref[row : row + TILE] = down
        row = 2 * HALO * TILE + side
        up_ref[row : row + 1] = ref[flags + size_z // TILE - 1 : flags + size_z // TILE]
        down_ref[row : row + 1] = ref[flags : flags + 1]


def main_kernel(
    dims, unroll, ls_ref, div_ref, act_ref, xl_ref, xh_ref, zl_ref, zh_ref, cl_ref, ch_ref,
    z_out, q_out, r_out, w_out, t_out, sums_out,
    open_ref, dist_ref, open5_ref, src_ref, gain_ref, va_ref, vb_ref, u_ref, dots_ref,
):
    size_x, size_z, size_y = dims
    ext_z = size_z + TILE
    deep = HALO + 1
    tiles_z = size_z // TILE
    tile_rows = rows_of((TILE, size_y))
    high_half = tile_rows < HALO

    def spread(row):
        return jnp.broadcast_to(row, (TILE, size_y))

    def split(levels, act):
        fluid = jnp.logical_and(levels < 0, act > 0)
        away = jnp.abs(levels)
        return jnp.where(fluid, 0.0, away), jnp.where(fluid, away, 0.0)

    def put(slot, z0, levels, act):
        open_tile, dist_tile = split(levels, act)
        open_ref[slot, z0 : z0 + TILE] = open_tile
        dist_ref[slot, z0 : z0 + TILE] = dist_tile

    def own_plane(x):
        tile_x = lax.div(x, TILE)
        for j in range(tiles_z):
            rows = slice(j * TILE, (j + 1) * TILE)
            put(x + deep, j * TILE, ls_ref[x, rows], spread(act_ref[j, pl.ds(tile_x, 1)]))
            src_ref[x + HALO, rows] = div_ref[x, rows]
        row = pl.multiple_of(x * TILE, TILE)
        from_low = zl_ref[pl.ds(row, TILE)]
        from_high = zh_ref[pl.ds(row, TILE)]
        flags = size_x * (TILE + 1) + tile_x
        act = jnp.where(
            high_half, spread(zh_ref[pl.ds(flags, 1)]), spread(zl_ref[pl.ds(flags, 1)])
        )
        put(x + deep, size_z, jnp.where(high_half, from_high, from_low), act)
        src_ref[x + HALO, size_z:ext_z] = swap_halves(jnp.where(high_half, from_low, from_high))
        fifth = size_x * TILE + x
        levels5 = jnp.where(
            high_half, spread(zh_ref[pl.ds(fifth, 1)]), spread(zl_ref[pl.ds(fifth, 1)])
        )
        open5_ref[x + HALO] = split(levels5, act)[0]


    fields = deep * size_z
    flags = (deep + HALO) * size_z
    for side, ref in ((0, xl_ref), (1, xh_ref)):
        for p in range(deep):
            slot = p + side * (size_x + deep)
            for j in range(tiles_z):
                row = p * size_z + j * TILE
                put(slot, j * TILE, ref[row : row + TILE], spread(ref[flags + j : flags + j + 1]))
        open_ref[0 if side == 0 else size_x + 2 * deep - 1, size_z:ext_z] = jnp.zeros((TILE, size_y), f32)
        flag = 2 * HALO * TILE + side
        act = jnp.where(high_half, spread(ch_ref[flag : flag + 1]), spread(cl_ref[flag : flag + 1]))
        for p in range(HALO):
            slot = p + side * (size_x + HALO)
            row = fields + p * size_z
            src_ref[slot, 0:size_z] = ref[row : row + size_z]
            row = (side * HALO + p) * TILE
            from_low = cl_ref[row : row + TILE]
            from_high = ch_ref[row : row + TILE]
            put(slot + 1, size_z, jnp.where(high_half, from_high, from_low), act)
            src_ref[slot, size_z:ext_z] = swap_halves(jnp.where(high_half, from_low, from_high))
            open5_ref[slot] = jnp.zeros((TILE, size_y), f32)

    lane_row = lax.broadcasted_iota(jnp.int32, (ext_z, LANES), 1)
    first_lane = lane_row == 0
    last_lane = lane_row == LANES - 1

    def along_y(v):
        right = pltpu.roll(v, size_y - 1, 1)
        left = pltpu.roll(v, 1, 1)
        cut = size_y - LANES
        right = jnp.concatenate([right[:, :cut], jnp.where(last_lane, 0.0, right[:, cut:])], 1)
        left = jnp.concatenate([jnp.where(first_lane, 0.0, left[:, :LANES]), left[:, LANES:]], 1)
        return right, left

    def along_z(v):
        return pltpu.roll(v, ext_z - 1, 0), pltpu.roll(v, 1, 0)

    def near(ref, slot):
        v = ref[slot]
        above, below = along_z(v)
        right, left = along_y(v)
        return (ref[slot + 1] + ref[slot - 1]) + (above + below) + (right + left)

    def gain_plane(slot):
        v = open_ref[slot + 1]
        above, below = along_z(v)
        right, left = along_y(v)
        beyond = open5_ref[slot]
        above = jnp.concatenate(
            [above[:size_z], jnp.where(tile_rows == HALO - 1, beyond, above[size_z:])], 0
        )
        below = jnp.concatenate(
            [below[:size_z], jnp.where(tile_rows == HALO, beyond, below[size_z:])], 0
        )
        dist = dist_ref[slot + 1]
        top = (ratio_cap - 1.0) * dist
        total = jnp.minimum(open_ref[slot + 2], top) + jnp.minimum(open_ref[slot], top)
        for piece in (above, below, right, left):
            total = total + jnp.minimum(piece, top)
        whole = jnp.where(dist > 0, 6.0 * dist + total, 1.0)
        gain = damping * dist / whole
        gain_ref[slot] = gain
        va_ref[slot] = gain * src_ref[slot]

    def folded(product):
        parts = [
            product[z0 : z0 + TILE, y0 : y0 + LANES]
            for z0 in range(0, size_z, TILE)
            for y0 in range(0, size_y, LANES)
        ]
        while len(parts) > 1:
            parts = [sum(parts[k + 1 : k + 2], parts[k]) for k in range(0, len(parts), 2)]
        return parts[0]

    def smooth_first(slot, own):
        u = (2.0 * damping) * src_ref[slot] + near(va_ref, slot)
        u_ref[slot] = u
        z = gain_ref[slot] * u
        vb_ref[slot] = z
        if own:
            z_out[slot - HALO] = z[:size_z]

    def image_first(slot, own):
        w = damping * u_ref[slot] - near(vb_ref, slot)
        u_ref[slot] = w
        gain = gain_ref[slot]
        va_ref[slot] = gain * w
        if own:
            fluid = gain[:size_z] > 0
            w = jnp.where(fluid, w[:size_z], 0.0)
            r = jnp.where(fluid, src_ref[slot, 0:size_z], 0.0)
            z = vb_ref[slot, 0:size_z]
            w_out[slot - HALO] = w
            r_out[slot - HALO] = r
            dots_ref[0] += folded(r * z)
            dots_ref[1] += folded(z * w)

    def smooth_second(slot):
        u = (2.0 * damping) * u_ref[slot] + near(va_ref, slot)
        u_ref[slot] = u
        vb_ref[slot] = gain_ref[slot] * u

    def image_second(slot):
        t = (damping * u_ref[slot] - near(vb_ref, slot))[:size_z]
        q = vb_ref[slot, 0:size_z]
        t = jnp.where(gain_ref[slot, 0:size_z] > 0, t, 0.0)
        q_out[slot - HALO] = q
        t_out[slot - HALO] = t
        dots_ref[2] += folded(w_out[slot - HALO] * q)
        dots_ref[3] += folded(q * t)

    def each(first, last, stage, *more):
        def body(slot, carry):
            stage(slot, *more)
            return carry

        if last > first:
            lax.fori_loop(first, last, body, 0, unroll=min(unroll, last - first))

    dots_ref[...] = jnp.zeros_like(dots_ref)
    ext_x = size_x + 2 * HALO
    lead = 3 * HALO
    stop = size_x + 2
    each(0, lead - 2, own_plane)
    each(0, lead, gain_plane)
    each(1, HALO, smooth_first, False)
    each(HALO, lead - 2, smooth_first, True)
    each(2, HALO, image_first, False)
    each(HALO, lead - 4, image_first, True)
    each(3, lead - 6, smooth_second)

    def sweep(i, carry):
        image_second(i - 8)
        smooth_second(i - 6)
        image_first(i - 4, True)
        smooth_first(i - 2, True)
        gain_plane(i)
        own_plane(i - 2)
        return carry

    lax.fori_loop(lead, stop, sweep, 0)
    each(stop, ext_x, gain_plane)
    each(stop - 2, ext_x - HALO, smooth_first, True)
    each(ext_x - HALO, ext_x - 1, smooth_first, False)
    each(stop - 4, ext_x - HALO, image_first, True)
    each(ext_x - HALO, ext_x - 2, image_first, False)
    each(stop - 6, ext_x - 3, smooth_second)
    each(stop - 8, ext_x - HALO, image_second)
    gamma, delta, cross, last = [dots_ref[k] for k in range(4)]

    lane = lax.broadcasted_iota(jnp.int32, (1, LANES), 1)
    line = jnp.zeros((1, LANES), f32)
    for place, part in enumerate((gamma, delta, cross, last)):
        line = jnp.where(lane == place, jnp.sum(part), line)
    sums_out[...] = jnp.broadcast_to(line, sums_out.shape)


def final_kernel(sums_ref, z_ref, q_ref, r_ref, w_ref, t_ref, pressure_ref, residual_ref):
    totals = jnp.sum(sums_ref[...], axis=0, keepdims=True)
    lane = lax.broadcasted_iota(jnp.int32, totals.shape, 1)
    gamma, delta, cross, last = [
        jnp.sum(jnp.where(lane == place, totals, 0.0), axis=1, keepdims=True) for place in range(4)
    ]
    alpha = gamma / delta
    gamma_next = gamma - 2.0 * alpha * delta + alpha * alpha * cross
    beta = gamma_next / gamma
    delta_next = delta - 2.0 * alpha * cross + alpha * alpha * last
    alpha_next = gamma_next / (delta_next - beta * gamma_next / alpha)
    on_first = (alpha + alpha_next * (1.0 + beta)).reshape(1, 1, 1)
    on_second = (-alpha_next * alpha).reshape(1, 1, 1)
    pressure_ref[...] = on_first * z_ref[...] + on_second * q_ref[...]
    residual_ref[...] = r_ref[...] - on_first * w_ref[...] - on_second * t_ref[...]


def shift(values, axis, step):
    count = lax.axis_size(axis)
    pairs = [(i, i + step) for i in range(count) if 0 <= i + step < count]
    return lax.ppermute(values, axis, pairs)


def array(*shape):
    return jax.ShapeDtypeStruct(shape, f32)


def on_device(divergence, level_set, tile_ids):
    dims = divergence.shape
    size_x, size_z, size_y = dims
    deep = HALO + 1
    tiles_x = size_x // TILE
    tiles_z = size_z // TILE
    hbm = pl.BlockSpec(memory_space=pltpu.HBM)

    x_rows = (deep + HALO) * size_z + TILE
    up_x, down_x, act = pl.pallas_call(
        functools.partial(pack_x_kernel, dims),
        out_shape=(array(x_rows, size_y), array(x_rows, size_y), array(tiles_z, tiles_x, size_y)),
        in_specs=[hbm, hbm, hbm],
        out_specs=(VMEM_SPEC,) * 3,
        scratch_shapes=[
            pltpu.VMEM((2 * (deep + HALO), size_z, size_y), f32),
            pltpu.VMEM(tile_ids.shape, jnp.int32),
            pltpu.SemaphoreType.DMA((5,)),
        ],
        compiler_params=pltpu.CompilerParams(vmem_limit_bytes=60 << 20),
        name="pack_x",
    )(tile_ids, level_set, divergence)
    x_low = shift(up_x, "gx", 1)
    x_high = shift(down_x, "gx", -1)

    planes = TILE
    z_rows = size_x * (TILE + 1) + max(tiles_x, TILE)
    whole = pl.BlockSpec((z_rows, size_y), lambda i: (0, 0))
    block = pl.BlockSpec((planes, size_z, size_y), lambda i: (i, 0, 0))
    up_z, down_z = pl.pallas_call(
        functools.partial(pack_z_kernel, dims, planes),
        grid=(size_x // planes,),
        out_shape=(array(z_rows, size_y),) * 2,
        in_specs=[block, block, pl.BlockSpec((tiles_z, tiles_x, size_y), lambda i: (0, 0, 0))],
        out_specs=(whole, whole),
        scratch_shapes=[pltpu.VMEM((planes, size_y), f32)] * 2,
        compiler_params=pltpu.CompilerParams(vmem_limit_bytes=8 << 20),
        name="pack_z",
    )(level_set, divergence, act)
    z_low = shift(up_z, "gz", 1)
    z_high = shift(down_z, "gz", -1)

    c_rows = 2 * HALO * TILE + TILE
    up_c, down_c = pl.pallas_call(
        functools.partial(pack_corner_kernel, dims),
        out_shape=(array(c_rows, size_y),) * 2,
        in_specs=[VMEM_SPEC] * 2,
        out_specs=(VMEM_SPEC,) * 2,
        compiler_params=pltpu.CompilerParams(vmem_limit_bytes=8 << 20),
        name="pack_corner",
    )(x_low, x_high)
    c_low = shift(up_c, "gz", 1)
    c_high = shift(down_c, "gz", -1)

    devices = lax.axis_size("gx") * lax.axis_size("gz")
    ext_x, ext_z = size_x + 2 * HALO, size_z + TILE
    field = pltpu.VMEM((ext_x, ext_z, size_y), f32)
    wide = pltpu.VMEM((ext_x + 2, ext_z, size_y), f32)
    z, q, r, w, t, sums = pl.pallas_call(
        functools.partial(main_kernel, dims, 3),
        out_shape=(array(*dims),) * 5 + (array(devices, LANES),),
        in_specs=[VMEM_SPEC] * 9,
        out_specs=(VMEM_SPEC,) * 6,
        scratch_shapes=[wide, wide, pltpu.VMEM((ext_x, TILE, size_y), f32)] + [field] * 5
        + [pltpu.VMEM((4, TILE, LANES), f32)],
        compiler_params=pltpu.CompilerParams(vmem_limit_bytes=30 << 20),
        name="cg_vectors",
    )(level_set, divergence, act, x_low, x_high, z_low, z_high, c_low, c_high)

    gathered = lax.all_to_all(sums, ("gx", "gz"), 0, 0, tiled=True)
    return tuple(
        pl.pallas_call(
            final_kernel,
            grid=(size_x // planes,),
            out_shape=(array(*dims),) * 2,
            in_specs=[pl.BlockSpec((devices, LANES), lambda i: (0, 0))] + [block] * 5,
            out_specs=(block,) * 2,
            compiler_params=pltpu.CompilerParams(vmem_limit_bytes=8 << 20),
            name="outputs",
        )(gathered, z, q, r, w, t)
    )


def solution(mesh):
    placed = (P("gx", "gz", None), P("gx", "gz", None), P("gx", "gz"))
    return jax.shard_map(
        on_device,
        mesh=mesh,
        in_specs=placed,
        out_specs=(P("gx", "gz", None), P("gx", "gz", None)),
        check_vma=False,
    )
```

```python
import functools

import jax
import jax.numpy as jnp
from jax import lax
from jax.experimental import pallas as pl
from jax.experimental.pallas import tpu as pltpu
from jax.sharding import PartitionSpec as P


TILE = 8
LANES = 128
HALO = 4
DEEP = HALO + 1
damping = 2.0 / 3.0
ratio_cap = 20.0
f32 = jnp.float32

VMEM_SPEC = pl.BlockSpec(memory_space=pltpu.VMEM)
HBM_SPEC = pl.BlockSpec(memory_space=pltpu.HBM)


ORIGIN = 12
ROWS = 24
RING = 16


def limit(mib):
    return pltpu.CompilerParams(vmem_limit_bytes=mib << 20)


def array(*shape):
    return jax.ShapeDtypeStruct(shape, f32)


def by_parity(axis, body):
    odd = lax.rem(lax.axis_index(axis), 2)

    @pl.when(odd == 0)
    def _():
        body(0)

    @pl.when(odd == 1)
    def _():
        body(1)


def flags_kernel(dims, ids_ref, act_ref):
    size_x, size_z, size_y = dims
    tiles_x, tiles_z, tiles_y = size_x // TILE, size_z // TILE, size_y // TILE
    ids = ids_ref[...]
    slots = ids.shape[1]
    column = lax.div(lax.broadcasted_iota(jnp.int32, (size_y, slots), 0), TILE)
    along_y = (column == lax.rem(ids, tiles_y)).astype(f32).astype(jnp.bfloat16)
    first = lax.broadcasted_iota(jnp.int32, (tiles_x, slots), 0) * (tiles_z * tiles_y)
    for layer in range(tiles_z):
        low = first + layer * tiles_y
        mine = jnp.logical_and(ids >= low, ids < low + tiles_y).astype(f32).astype(jnp.bfloat16)
        act_ref[layer] = lax.dot_general(
            mine, along_y, (((1,), (1,)), ((), ())), preferred_element_type=f32
        )


def pair(first_rows, low_ls, high_ls, low_div, high_div):
    up = jnp.where(first_rows, pltpu.roll(high_div, HALO, 0), high_ls)
    down = jnp.where(first_rows, low_ls, pltpu.roll(low_div, HALO, 0))
    return up, down


def pack_x_kernel(dims, ids_hbm, ls_hbm, div_hbm, even_ref, odd_ref, act_ref, ids, buf, sems):
    size_x, size_z, _ = dims
    tiles_x, tiles_z = size_x // TILE, size_z // TILE
    ids_copy = pltpu.make_async_copy(ids_hbm, ids, sems.at[4])
    ids_copy.start()
    copies = []
    for source, first, count, place in (
        (ls_hbm, size_x - DEEP, DEEP, 0),
        (div_hbm, size_x - HALO, HALO, DEEP),
        (ls_hbm, 0, DEEP, DEEP + HALO),
        (div_hbm, 0, HALO, 2 * DEEP + HALO),
    ):
        copy = pltpu.make_async_copy(
            source.at[pl.ds(first, count)], buf.at[pl.ds(place, count)], sems.at[len(copies)]
        )
        copy.start()
        copies.append(copy)
    ids_copy.wait()
    flags_kernel(dims, ids, act_ref)
    for copy in copies:
        copy.wait()

    def put(odd):
        for ref, place, tile_x in zip((even_ref, odd_ref), (odd, 1 - odd), (0, 0)):
            tile_x = tiles_x - 1 if place == 0 else 0
            for p in range(DEEP + HALO):
                ref[p * size_z : (p + 1) * size_z] = buf[place * (DEEP + HALO) + p]
            flags = (DEEP + HALO) * size_z
            for layer in range(tiles_z):
                ref[flags + layer : flags + layer + 1] = act_ref[layer, tile_x : tile_x + 1]

    by_parity("gx", put)


def pack_z_kernel(dims, parts, ls_ref, div_ref, act_ref, *refs):
    _, size_z, size_y = dims
    tiles_z = size_z // TILE
    first_rows = lax.broadcasted_iota(jnp.int32, (TILE, size_y), 0) < HALO
    top = slice(size_z - TILE, size_z)

    def put(odd):
        for part, (base, span) in enumerate(parts):
            even_ref, odd_ref = refs[2 * part], refs[2 * part + 1]
            up_z, down_z = (even_ref, odd_ref) if odd == 0 else (odd_ref, even_ref)

            def planes(x0, carry):
                fifth_up, fifth_down = [], []
                for p in range(TILE):
                    x = base + x0 * TILE + p
                    low_ls, high_ls = ls_ref[x, 0:TILE], ls_ref[x, top]
                    up, down = pair(first_rows, low_ls, high_ls, div_ref[x, 0:TILE], div_ref[x, top])
                    row = pl.multiple_of((x - base) * TILE, TILE)
                    up_z[pl.ds(row, TILE)] = up
                    down_z[pl.ds(row, TILE)] = down
                    fifth_up.append(high_ls[TILE - DEEP : TILE - HALO])
                    fifth_down.append(low_ls[HALO:DEEP])
                row = pl.multiple_of((span + x0) * TILE, TILE)
                up_z[pl.ds(row, TILE)] = jnp.concatenate(fifth_up, 0)
                down_z[pl.ds(row, TILE)] = jnp.concatenate(fifth_down, 0)
                return carry

            lax.fori_loop(0, span // TILE, planes, 0)
            flags, tiles = span * (TILE + 1), slice(base // TILE, (base + span) // TILE)
            up_z[flags : flags + span // TILE] = act_ref[tiles_z - 1, tiles]
            down_z[flags : flags + span // TILE] = act_ref[0, tiles]

    by_parity("gz", put)


def pack_corner_kernel(dims, x_even, x_odd, after_ref, even_ref, odd_ref):
    del after_ref
    _, size_z, size_y = dims
    tiles_z = size_z // TILE
    first_rows = lax.broadcasted_iota(jnp.int32, (TILE, size_y), 0) < HALO
    flags = (DEEP + HALO) * size_z

    def put(odd_x):
        low, high = (x_odd, x_even) if odd_x == 0 else (x_even, x_odd)

        def put_z(odd_z):
            up_ref, down_ref = (even_ref, odd_ref) if odd_z == 0 else (odd_ref, even_ref)
            for side, ref in enumerate((low, high)):
                for p in range(HALO):
                    ls_row = (p + 1 - side) * size_z
                    div_row = (DEEP + p) * size_z
                    up, down = pair(
                        first_rows,
                        ref[ls_row : ls_row + TILE],
                        ref[ls_row + size_z - TILE : ls_row + size_z],
                        ref[div_row : div_row + TILE],
                        ref[div_row + size_z - TILE : div_row + size_z],
                    )
                    row = (side * HALO + p) * TILE
                    up_ref[row : row + TILE] = up
                    down_ref[row : row + TILE] = down
                row = 2 * HALO * TILE + side
                up_ref[row : row + 1] = ref[flags + tiles_z - 1 : flags + tiles_z]
                down_ref[row : row + 1] = ref[flags : flags + 1]

        by_parity("gz", put_z)

    by_parity("gx", put)


class Stages:
    def __init__(self, dims, ring, open_ref, dist_ref, src_ref, gain_ref, va_ref, vb_ref, u_ref):
        self.ring = ring
        self.size_x, self.size_z, self.size_y = dims
        self.count = self.size_y // LANES
        self.open, self.dist, self.src, self.gain = open_ref, dist_ref, src_ref, gain_ref
        self.va, self.vb, self.u = va_ref, vb_ref, u_ref
        self.low, self.wide = ORIGIN - HALO, self.size_z + 2 * HALO
        self.tile_rows = lax.broadcasted_iota(jnp.int32, (TILE, self.size_y), 0)

    def at(self, slot):
        return jnp.bitwise_and(slot, self.ring - 1) if self.ring else slot

    def chunk(self, c):
        return slice(c * LANES, (c + 1) * LANES)

    def put(self, slot, row, levels, act):
        slot = self.at(slot)
        fluid = jnp.logical_and(levels < 0, act > 0)
        away = jnp.abs(levels)
        opened = jnp.where(fluid, 0.0, away)
        dist = jnp.where(fluid, away, 0.0)
        for c in range(self.count):
            self.open[slot, c, row : row + TILE] = opened[:, self.chunk(c)]
            self.dist[slot, c, row : row + TILE] = dist[:, self.chunk(c)]

    def put_source(self, slot, row, values):
        slot = self.at(slot)
        for c in range(self.count):
            self.src[slot, c, row : row + values.shape[0]] = values[:, self.chunk(c)]

    def spread(self, row):
        return jnp.broadcast_to(row, (TILE, self.size_y))

    def own_plane(self, slot, x, ls_ref, div_ref, act_ref, zl_ref, zh_ref, base, span):
        size_z = self.size_z
        tile_x = lax.div(x, TILE)
        row = (x - base) * TILE
        row = row if isinstance(x, int) else pl.multiple_of(row, TILE)
        flag, fifth = span * (TILE + 1) + tile_x - base // TILE, span * TILE + x - base
        below, above = zl_ref[pl.ds(row, TILE)], zh_ref[pl.ds(row, TILE)]
        self.put_source(slot, ORIGIN - HALO, below)
        self.put_source(slot, ORIGIN + size_z - HALO, above)
        self.put_source(slot, ORIGIN, div_ref[x])
        below = jnp.where(self.tile_rows == HALO - 1, self.spread(zl_ref[pl.ds(fifth, 1)]), below)
        above = jnp.where(self.tile_rows == HALO, self.spread(zh_ref[pl.ds(fifth, 1)]), above)
        self.put(slot, ORIGIN - TILE, below, self.spread(zl_ref[pl.ds(flag, 1)]))
        self.put(slot, ORIGIN + size_z, above, self.spread(zh_ref[pl.ds(flag, 1)]))
        for j in range(size_z // TILE):
            rows = slice(j * TILE, (j + 1) * TILE)
            self.put(slot, ORIGIN + j * TILE, ls_ref[x, rows], self.spread(act_ref[j, pl.ds(tile_x, 1)]))

    def lateral(self, values):
        lane = lax.broadcasted_iota(jnp.int32, values[0].shape, 1)
        first, last = lane == 0, lane == LANES - 1
        left = [pltpu.roll(v, 1, 1) for v in values]
        right = [pltpu.roll(v, LANES - 1, 1) for v in values]
        lefts = [jnp.where(first, left[c - 1] if c else 0.0, left[c]) for c in range(self.count)]
        rights = [
            jnp.where(last, right[c + 1] if c + 1 < self.count else 0.0, right[c])
            for c in range(self.count)
        ]
        return lefts, rights

    def near(self, ref, slot, low, wide):
        rows = slice(low, low + wide)
        here, before, after = self.at(slot), self.at(slot - 1), self.at(slot + 1)
        lefts, rights = self.lateral([ref[here, c, rows] for c in range(self.count)])
        return [
            (ref[after, c, rows] + ref[before, c, rows])
            + (ref[here, c, low + 1 : low + wide + 1] + ref[here, c, low - 1 : low + wide - 1])
            + (lefts[c] + rights[c])
            for c in range(self.count)
        ]

    def gains(self, slot):
        low, wide, ref = self.low, self.wide, self.open
        rows = slice(low, low + wide)
        before, after, slot = self.at(slot - 1), self.at(slot + 1), self.at(slot)
        lefts, rights = self.lateral([ref[slot, c, rows] for c in range(self.count)])
        for c in range(self.count):
            dist = self.dist[slot, c, rows]
            top = (ratio_cap - 1.0) * dist
            pieces = [
                jnp.minimum(piece, top)
                for piece in (
                    ref[after, c, rows],
                    ref[before, c, rows],
                    ref[slot, c, low + 1 : low + wide + 1],
                    ref[slot, c, low - 1 : low + wide - 1],
                    lefts[c],
                    rights[c],
                )
            ]
            total = (pieces[0] + pieces[1]) + (pieces[2] + pieces[3]) + (pieces[4] + pieces[5])
            whole = jnp.where(dist > 0, 6.0 * dist + total, 1.0)
            gain = damping * dist / whole
            self.gain[slot, c, rows] = gain
            self.va[slot, c, rows] = gain * self.src[slot, c, rows]

    def smooth_first(self, slot):
        rows = slice(self.low, self.low + self.wide)
        around = self.near(self.va, slot, self.low, self.wide)
        slot = self.at(slot)
        for c in range(self.count):
            u = (2.0 * damping) * self.src[slot, c, rows] + around[c]
            self.u[slot, c, rows] = u
            self.vb[slot, c, rows] = self.gain[slot, c, rows] * u

    def image_first(self, slot):
        rows = slice(self.low, self.low + self.wide)
        around = self.near(self.vb, slot, self.low, self.wide)
        slot = self.at(slot)
        for c in range(self.count):
            w = damping * self.u[slot, c, rows] - around[c]
            self.u[slot, c, rows] = w
            self.va[slot, c, rows] = self.gain[slot, c, rows] * w

    def keep_first(self, slot, x, place, div_ref, z_out, r_out, w_out, dots):
        own = slice(ORIGIN, ORIGIN + self.size_z)
        slot = self.at(slot)
        gamma, delta = [], []
        for c in range(self.count):
            ch = self.chunk(c)
            fluid = self.gain[slot, c, own] > 0
            z = self.vb[slot, c, own]
            r = jnp.where(fluid, div_ref[x, :, ch], 0.0)
            w = jnp.where(fluid, self.u[slot, c, own], 0.0)
            z_out[place + (slice(None), ch)] = z
            r_out[place + (slice(None), ch)] = r
            w_out[place + (slice(None), ch)] = w
            gamma.append(r * z)
            delta.append(z * w)
        dots[0] += self.folded(gamma)
        dots[1] += self.folded(delta)

    def smooth_second(self, slot):
        rows = slice(self.low, self.low + self.wide)
        around = self.near(self.va, slot, self.low, self.wide)
        slot = self.at(slot)
        for c in range(self.count):
            u = (2.0 * damping) * self.u[slot, c, rows] + around[c]
            self.u[slot, c, rows] = u
            self.vb[slot, c, rows] = self.gain[slot, c, rows] * u

    def image_second(self, slot, place, w_ref, w_place, q_out, t_out, dots):
        own = slice(ORIGIN, ORIGIN + self.size_z)
        around = self.near(self.vb, slot, ORIGIN, self.size_z)
        slot = self.at(slot)
        cross, last = [], []
        for c in range(self.count):
            ch = self.chunk(c)
            t = damping * self.u[slot, c, own] - around[c]
            t = jnp.where(self.gain[slot, c, own] > 0, t, 0.0)
            q = self.vb[slot, c, own]
            q_out[place + (slice(None), ch)] = q
            t_out[place + (slice(None), ch)] = t
            cross.append(w_ref[w_place + (slice(None), ch)] * q)
            last.append(q * t)
        dots[2] += self.folded(cross)
        dots[3] += self.folded(last)

    def folded(self, products):
        parts = [
            product[z0 : z0 + TILE] for product in products for z0 in range(0, self.size_z, TILE)
        ]
        while len(parts) > 1:
            parts = [sum(parts[k + 1 : k + 2], parts[k]) for k in range(0, len(parts), 2)]
        return parts[0]

    def handed(self):
        return (
            [(self.va, m) for m in range(1, 5)]
            + [(self.vb, m) for m in range(2, 6)]
            + [(self.u, m) for m in range(2, 5)]
            + [(self.gain, m) for m in range(1, 5)]
            + [(self.src, 1)]
        )


HANDED = 16


LEAD = 13
EDGE = 5


def each(first, end, stage, unroll=3):
    def body(x, carry):
        stage(x)
        return carry

    lax.fori_loop(first, end, body, 0, unroll=min(unroll, end - first))


def inner_steps(do, part, ls_ref, div_ref, act_ref, zl_ref, zh_ref, outs, dots):
    z_out, q_out, r_out, w_out, t_out = outs

    def own(x):
        do.own_plane(x, x, ls_ref, div_ref, act_ref, zl_ref, zh_ref, *part)

    def second(x):
        do.keep_first(x, x, (x,), div_ref, z_out, r_out, w_out, dots)
        do.smooth_second(x)

    def last(x):
        do.image_second(x, (x,), w_out, (x,), q_out, t_out, dots)

    def sweep(i):
        last(i - 8)
        second(i - 6)
        do.image_first(i - 4)
        do.smooth_first(i - 2)
        do.gains(i)
        own(i + 2)

    return own, second, last, sweep


def inner_first_kernel(dims, part, ls_ref, div_ref, act_ref, z_even, z_odd, *outs):
    vectors, hand_out, dots, fields = outs[:5], outs[5], outs[6], outs[7:]

    def run(odd):
        low, high = (z_odd, z_even) if odd == 0 else (z_even, z_odd)
        do = Stages(dims, RING, *fields)
        dots[...] = jnp.zeros_like(dots)
        own, second, _, sweep = inner_steps(
            do, part, ls_ref, div_ref, act_ref, low, high, vectors, dots
        )
        each(0, LEAD + 2, own)
        each(1, LEAD, do.gains)
        each(2, LEAD - 2, do.smooth_first)
        each(3, LEAD - 4, do.image_first)
        each(4, LEAD - 6, second)
        for item, (ref, m) in enumerate(do.handed()):
            hand_out[item] = ref[m]
        each(LEAD, part[1] - 2, sweep, 1)

    by_parity("gz", run)


def inner_last_kernel(
    dims, part, ls_ref, div_ref, act_ref, z_even, z_odd, w_first, dots_first, *refs
):
    held, vectors, hand_out, dots, fields = refs[:7], refs[7:12], refs[12], refs[13], refs[14:]
    size_x = dims[0]
    start, stop = part[0] - 2, size_x - 2

    def run(odd):
        low, high = (z_odd, z_even) if odd == 0 else (z_even, z_odd)
        do = Stages(dims, RING, *fields)
        dots[...] = dots_first[...]
        for ref, old, first, end in zip(
            fields, held, (-1, 0, -2, -8, -7, -9, -8), (2, 2, 2, 0, 0, -2, -2)
        ):
            for x in range(start + first, start + end):
                ref[x % RING] = old[x % RING]
        for x in range(start - 8, start - 6):
            vectors[3][x] = w_first[x]
        _, second, last, sweep = inner_steps(
            do, part, ls_ref, div_ref, act_ref, low, high, vectors, dots
        )
        each(start, stop, sweep, 1)
        each(stop, size_x - 1, do.gains)
        each(stop - 2, size_x - 2, do.smooth_first)
        each(stop - 4, size_x - 3, do.image_first)
        each(stop - 6, size_x - 4, second)
        each(stop - 8, size_x - 5, last)
        for item, (ref, m) in enumerate(do.handed()):
            hand_out[item] = ref[do.at(size_x - 1 - m)]

    by_parity("gz", run)


SPAN = 12


def ends_kernel(
    dims, parts, ls_ref, div_ref, act_ref, z_first_even, z_first_odd, z_last_even, z_last_odd, x_even, x_odd, c_even, c_odd,
    hand_low, hand_high, w_low, w_high, inner_dots, z_out, q_out, r_out, w_out, t_out, sums_out, dots, *fields,
):
    size_x, size_z, _ = dims
    z_first, z_last = (z_first_even, z_first_odd), (z_last_even, z_last_odd)
    do = Stages(dims, 0, *fields)
    dots[...] = inner_dots[...]

    def slot(side, m):
        return side * SPAN + m + DEEP

    def x_of(side, m):
        return m if side == 0 else size_x - 1 - m

    for side in range(2):
        for item, (ref, m) in enumerate(do.handed()):
            ref[slot(side, m)] = (hand_low, hand_high)[side][item]
        blank = jnp.zeros((TILE, LANES), f32)
        for c in range(do.count):
            do.open[slot(side, -DEEP), c, ORIGIN - TILE : ORIGIN] = blank
            do.open[slot(side, -DEEP), c, ORIGIN + size_z : ORIGIN + size_z + TILE] = blank

    def fill_z(odd):
        cl_ref, ch_ref = (c_odd, c_even) if odd == 0 else (c_even, c_odd)
        for side in range(2):
            z_even, z_odd = (z_first, z_last)[side]
            zl_ref, zh_ref = (z_odd, z_even) if odd == 0 else (z_even, z_odd)
            for m in range(2):
                do.own_plane(
                    slot(side, m), x_of(side, m), ls_ref, div_ref, act_ref, zl_ref, zh_ref, *parts[side]
                )
            flag = 2 * HALO * TILE + side
            for p in range(HALO):
                here = slot(side, p - HALO if side == 0 else -1 - p)
                row = (side * HALO + p) * TILE
                below, above = cl_ref[row : row + TILE], ch_ref[row : row + TILE]
                do.put_source(here, ORIGIN - HALO, below)
                do.put_source(here, ORIGIN + size_z - HALO, above)
                do.put(here, ORIGIN - TILE, below, do.spread(cl_ref[flag : flag + 1]))
                do.put(here, ORIGIN + size_z, above, do.spread(ch_ref[flag : flag + 1]))

    def fill_x(odd):
        for side, ref in enumerate((x_odd, x_even) if odd == 0 else (x_even, x_odd)):
            flags = (DEEP + HALO) * size_z
            for p in range(DEEP):
                here = slot(side, p - DEEP if side == 0 else -1 - p)
                for j in range(size_z // TILE):
                    row = p * size_z + j * TILE
                    act = do.spread(ref[flags + j : flags + j + 1])
                    do.put(here, ORIGIN + j * TILE, ref[row : row + TILE], act)
            for p in range(HALO):
                row = (DEEP + p) * size_z
                here = slot(side, p - HALO if side == 0 else -1 - p)
                do.put_source(here, ORIGIN, ref[row : row + size_z])

    by_parity("gz", fill_z)
    by_parity("gx", fill_x)

    def both(first, end, stage):
        def body(n, carry):
            for side in range(2):
                stage(side, side * SPAN + n, n - DEEP)
            return carry

        lax.fori_loop(first + DEEP, end + DEEP, body, 0)

    both(-4, 1, lambda side, here, m: do.gains(here))
    both(-3, 2, lambda side, here, m: do.smooth_first(here))
    both(-2, 3, lambda side, here, m: do.image_first(here))
    both(
        0, EDGE - 1,
        lambda side, here, m: do.keep_first(
            here, x_of(side, m), (side, m), div_ref, z_out, r_out, w_out, dots
        ),
    )
    for side in range(2):
        w_out[side, EDGE - 1] = (w_low, w_high)[side][x_of(side, EDGE - 1)]
    both(-1, 4, lambda side, here, m: do.smooth_second(here))
    both(
        0, EDGE,
        lambda side, here, m: do.image_second(
            here, (side, m), w_out, (side, m), q_out, t_out, dots
        ),
    )
    lane = lax.broadcasted_iota(jnp.int32, (1, LANES), 1)
    line = jnp.zeros((1, LANES), f32)
    for place in range(4):
        line = jnp.where(lane == place, jnp.sum(dots[place]), line)
    sums_out[...] = jnp.broadcast_to(line, sums_out.shape)


def final_kernel(
    planes, meet, sums_ref, *refs
):
    first, final, ends = refs[:5], refs[5:10], refs[10:15]
    pressure_out, residual_out, pressure, residual, sems = refs[15:]
    totals = jnp.sum(sums_ref[...], axis=0, keepdims=True)
    lane = lax.broadcasted_iota(jnp.int32, totals.shape, 1)
    gamma, delta, cross, last = [
        jnp.sum(jnp.where(lane == place, totals, 0.0), axis=1, keepdims=True) for place in range(4)
    ]
    alpha = gamma / delta
    gamma_next = gamma - 2.0 * alpha * delta + alpha * alpha * cross
    beta = gamma_next / gamma
    delta_next = delta - 2.0 * alpha * cross + alpha * alpha * last
    alpha_next = gamma_next / (delta_next - beta * gamma_next / alpha)
    size_x, _, size_y = pressure.shape
    on_first = jnp.broadcast_to(alpha + alpha_next * (1.0 + beta), (1, LANES))
    on_second = jnp.broadcast_to(-alpha_next * alpha, (1, LANES))
    on_first = jnp.concatenate([on_first] * (size_y // LANES), 1)
    on_second = jnp.concatenate([on_second] * (size_y // LANES), 1)

    def put(x, z, q, r, w, t):
        pressure[x] = on_first * z + on_second * q
        residual[x] = r - on_first * w - on_second * t

    late = (0, 2, 0, 0, 2)

    def one(x):
        edge = min(x, size_x - 1 - x)
        side = int(x >= size_x // 2)
        picked = []
        for k in range(5):
            if edge < (EDGE if late[k] else EDGE - 1):
                picked.append(ends[k][side, edge])
            else:
                picked.append((first if x < meet - late[k] else final)[k][x])
        put(x, *picked)

    for x in (*range(EDGE), meet - 2, meet - 1, *range(size_x - EDGE, size_x)):
        one(x)

    def from_first(x, carry):
        put(x, *(ref[x] for ref in first))
        return carry

    def from_final(x, carry):
        put(x, *(ref[x] for ref in final))
        return carry

    copies = []
    for chunk in range(size_x // planes):
        begin, end = chunk * planes, (chunk + 1) * planes
        for low, high, step in ((EDGE, meet - 2, from_first), (meet, size_x - EDGE, from_final)):
            low, high = max(begin, low), min(end, high)
            if low < high:
                lax.fori_loop(low, high, step, 0, unroll=min(4, high - low))
        where = pl.ds(begin, planes)
        for place, (src, dst) in enumerate(((pressure, pressure_out), (residual, residual_out))):
            copy = pltpu.make_async_copy(src.at[where], dst.at[where], sems.at[2 * chunk + place])
            copy.start()
            copies.append(copy)
    for copy in copies:
        copy.wait()


def exchange(values, axis, odd):
    count = lax.axis_size(axis)
    pairs = [(i, ((i - odd) ^ 1) + odd) for i in range(count)]
    return lax.ppermute(values, axis, [(i, j) for i, j in pairs if 0 <= j < count])


def on_device(divergence, level_set, tile_ids):
    dims = divergence.shape
    size_x, size_z, size_y = dims
    tiles_x, tiles_z = size_x // TILE, size_z // TILE
    count_x, count_z = lax.axis_size("gx"), lax.axis_size("gz")

    half = tiles_x // 2 * TILE
    parts = ((0, half), (half, size_x - half))
    z_rows = [span * TILE + span + -(-span // TILE // TILE) * TILE for _, span in parts]
    x_rows = (DEEP + HALO) * size_z + TILE
    c_rows = 2 * HALO * TILE + TILE
    x_even, x_odd, act = pl.pallas_call(
        functools.partial(pack_x_kernel, dims),
        out_shape=(array(x_rows, size_y),) * 2 + (array(tiles_z, tiles_x, size_y),),
        in_specs=[HBM_SPEC] * 3,
        out_specs=(VMEM_SPEC,) * 3,
        scratch_shapes=[
            pltpu.VMEM(tile_ids.shape, jnp.int32),
            pltpu.VMEM((2 * (DEEP + HALO), size_z, size_y), f32),
            pltpu.SemaphoreType.DMA((5,)),
        ],
        compiler_params=limit(57),
        name="pack_x",
    )(tile_ids, level_set, divergence)
    x_even = exchange(x_even, "gx", 0)
    x_odd = exchange(x_odd, "gx", 1)
    sent = pl.pallas_call(
        functools.partial(pack_z_kernel, dims, parts),
        out_shape=[array(rows, size_y) for rows in z_rows for _ in range(2)],
        in_specs=[VMEM_SPEC] * 3,
        out_specs=[VMEM_SPEC] * 4,
        compiler_params=limit(8),
        name="pack_z",
    )(level_set, divergence, act)
    z_first, z_last = [
        (exchange(sent[2 * part], "gz", 0), exchange(sent[2 * part + 1], "gz", 1))
        for part in range(2)
    ]

    def fields(planes):
        return [pltpu.VMEM((planes, size_y // LANES, size_z + ROWS, LANES), f32)] * 7

    block = array(*dims)
    chunks, rows = size_y // LANES, size_z + ROWS
    hand = array(HANDED, chunks, rows, LANES)
    dots = array(4, TILE, LANES)
    ring = [array(RING, chunks, rows, LANES)] * 7
    early = array(half, size_z, size_y)
    first_call = pl.pallas_call(
        functools.partial(inner_first_kernel, dims, parts[0]),
        out_shape=[early] * 5 + [hand, dots] + ring,
        in_specs=[VMEM_SPEC] * 5,
        out_specs=[VMEM_SPEC] * 14,
        compiler_params=limit(4),
        name="inner_first",
    )
    *first, hand_low, dots_first = (outs := first_call(level_set, divergence, act, *z_first))[:7]
    held = outs[7:]
    c_even, c_odd = pl.pallas_call(
        functools.partial(pack_corner_kernel, dims),
        out_shape=(array(c_rows, size_y),) * 2,
        in_specs=[VMEM_SPEC] * 3,
        out_specs=(VMEM_SPEC,) * 2,
        compiler_params=limit(8),
        name="pack_corner",
    )(x_even, x_odd, dots_first)
    c_odd = exchange(c_odd, "gz", 1)
    c_even = exchange(c_even, "gz", 0)

    last_call = pl.pallas_call(
        functools.partial(inner_last_kernel, dims, parts[1]),
        out_shape=[block] * 5 + [hand, dots],
        in_specs=[VMEM_SPEC] * 14,
        out_specs=[VMEM_SPEC] * 7,
        scratch_shapes=fields(RING),
        compiler_params=limit(12),
        name="inner_last",
    )
    *second, hand_high, dots_last = last_call(
        level_set, divergence, act, *z_last, first[3], dots_first, *held
    )

    devices = count_x * count_z
    end = array(2, EDGE, size_z, size_y)
    *ends, sums = pl.pallas_call(
        functools.partial(ends_kernel, dims, parts),
        out_shape=(end,) * 5 + (array(devices, LANES),),
        in_specs=[VMEM_SPEC] * 16,
        out_specs=(VMEM_SPEC,) * 6,
        scratch_shapes=[pltpu.VMEM((4, TILE, LANES), f32)] + fields(2 * SPAN),
        compiler_params=limit(20),
        name="ends",
    )(
        level_set, divergence, act, *z_first, *z_last, x_even, x_odd, c_even, c_odd,
        hand_low, hand_high, first[3], second[3], dots_last,
    )

    gathered = lax.all_to_all(sums, ("gx", "gz"), 0, 0, tiled=True)
    planes = TILE
    return tuple(
        pl.pallas_call(
            functools.partial(final_kernel, planes, half - 8),
            out_shape=(block,) * 2,
            in_specs=[VMEM_SPEC] * 16,
            out_specs=(HBM_SPEC,) * 2,
            scratch_shapes=[
                pltpu.VMEM(dims, f32),
                pltpu.VMEM(dims, f32),
                pltpu.SemaphoreType.DMA((2 * size_x // planes,)),
            ],
            compiler_params=limit(8),
            name="outputs",
        )(gathered, *first, *second, *ends)
    )


def solution(mesh):
    placed = (P("gx", "gz", None), P("gx", "gz", None), P("gx", "gz"))
    return jax.shard_map(
        on_device,
        mesh=mesh,
        in_specs=placed,
        out_specs=(P("gx", "gz", None), P("gx", "gz", None)),
        check_vma=False,
    )
```

```python
import functools

import jax
import jax.numpy as jnp
from jax import lax
from jax.experimental import pallas as pl
from jax.experimental.pallas import tpu as pltpu
from jax.sharding import PartitionSpec as P


TILE = 8
LANES = 128
HALO = 4
DEEP = HALO + 1
damping = 2.0 / 3.0
ratio_cap = 20.0
f32 = jnp.float32

VMEM_SPEC = pl.BlockSpec(memory_space=pltpu.VMEM)
HBM_SPEC = pl.BlockSpec(memory_space=pltpu.HBM)


ROWS = TILE
RING = 16


def limit(mib):
    return pltpu.CompilerParams(vmem_limit_bytes=mib << 20)


def array(*shape):
    return jax.ShapeDtypeStruct(shape, f32)


def by_parity(axis, body):
    odd = lax.rem(lax.axis_index(axis), 2)

    @pl.when(odd == 0)
    def _():
        body(0)

    @pl.when(odd == 1)
    def _():
        body(1)


def flags_kernel(dims, ids_ref, act_ref):
    size_x, size_z, size_y = dims
    tiles_x, tiles_z, tiles_y = size_x // TILE, size_z // TILE, size_y // TILE
    ids = ids_ref[...]
    slots = ids.shape[1]
    column = lax.div(lax.broadcasted_iota(jnp.int32, (size_y, slots), 0), TILE)
    along_y = (column == lax.rem(ids, tiles_y)).astype(f32).astype(jnp.bfloat16)
    first = lax.broadcasted_iota(jnp.int32, (tiles_x, slots), 0) * (tiles_z * tiles_y)
    for layer in range(tiles_z):
        low = first + layer * tiles_y
        mine = jnp.logical_and(ids >= low, ids < low + tiles_y).astype(f32).astype(jnp.bfloat16)
        act_ref[layer] = lax.dot_general(
            mine, along_y, (((1,), (1,)), ((), ())), preferred_element_type=f32
        )


def pair(first_rows, low_ls, high_ls, low_div, high_div):
    up = jnp.where(first_rows, pltpu.roll(high_div, HALO, 0), high_ls)
    down = jnp.where(first_rows, low_ls, pltpu.roll(low_div, HALO, 0))
    return up, down


def pack_x_kernel(dims, ids_hbm, ls_hbm, div_hbm, even_ref, odd_ref, act_ref, ids, buf, sems):
    size_x, size_z, _ = dims
    tiles_x, tiles_z = size_x // TILE, size_z // TILE
    ids_copy = pltpu.make_async_copy(ids_hbm, ids, sems.at[4])
    ids_copy.start()
    copies = []
    for source, first, count, place in (
        (ls_hbm, size_x - DEEP, DEEP, 0),
        (div_hbm, size_x - HALO, HALO, DEEP),
        (ls_hbm, 0, DEEP, DEEP + HALO),
        (div_hbm, 0, HALO, 2 * DEEP + HALO),
    ):
        copy = pltpu.make_async_copy(
            source.at[pl.ds(first, count)], buf.at[pl.ds(place, count)], sems.at[len(copies)]
        )
        copy.start()
        copies.append(copy)
    ids_copy.wait()
    flags_kernel(dims, ids, act_ref)
    for copy in copies:
        copy.wait()

    def put(odd):
        for ref, place, tile_x in zip((even_ref, odd_ref), (odd, 1 - odd), (0, 0)):
            tile_x = tiles_x - 1 if place == 0 else 0
            for p in range(DEEP + HALO):
                ref[p * size_z : (p + 1) * size_z] = buf[place * (DEEP + HALO) + p]
            flags = (DEEP + HALO) * size_z
            for layer in range(tiles_z):
                ref[flags + layer : flags + layer + 1] = act_ref[layer, tile_x : tile_x + 1]

    by_parity("gx", put)


def pack_z_kernel(dims, parts, ls_ref, div_ref, act_ref, *refs):
    _, size_z, size_y = dims
    tiles_z = size_z // TILE
    first_rows = lax.broadcasted_iota(jnp.int32, (TILE, size_y), 0) < HALO
    top = slice(size_z - TILE, size_z)

    def put(odd):
        for part, (base, span) in enumerate(parts):
            even_ref, odd_ref = refs[2 * part], refs[2 * part + 1]
            up_z, down_z = (even_ref, odd_ref) if odd == 0 else (odd_ref, even_ref)

            def planes(x0, carry):
                fifth_up, fifth_down = [], []
                for p in range(TILE):
                    x = base + x0 * TILE + p
                    low_ls, high_ls = ls_ref[x, 0:TILE], ls_ref[x, top]
                    up, down = pair(first_rows, low_ls, high_ls, div_ref[x, 0:TILE], div_ref[x, top])
                    row = pl.multiple_of((x - base) * TILE, TILE)
                    up_z[pl.ds(row, TILE)] = up
                    down_z[pl.ds(row, TILE)] = down
                    fifth_up.append(high_ls[TILE - DEEP : TILE - HALO])
                    fifth_down.append(low_ls[HALO:DEEP])
                row = pl.multiple_of((span + x0) * TILE, TILE)
                up_z[pl.ds(row, TILE)] = jnp.concatenate(fifth_up, 0)
                down_z[pl.ds(row, TILE)] = jnp.concatenate(fifth_down, 0)
                return carry

            lax.fori_loop(0, span // TILE, planes, 0)
            flags, tiles = span * (TILE + 1), slice(base // TILE, (base + span) // TILE)
            up_z[flags : flags + span // TILE] = act_ref[tiles_z - 1, tiles]
            down_z[flags : flags + span // TILE] = act_ref[0, tiles]

    by_parity("gz", put)


def pack_corner_kernel(dims, x_even, x_odd, after_ref, even_ref, odd_ref):
    del after_ref
    _, size_z, size_y = dims
    tiles_z = size_z // TILE
    first_rows = lax.broadcasted_iota(jnp.int32, (TILE, size_y), 0) < HALO
    flags = (DEEP + HALO) * size_z

    def put(odd_x):
        low, high = (x_odd, x_even) if odd_x == 0 else (x_even, x_odd)

        def put_z(odd_z):
            up_ref, down_ref = (even_ref, odd_ref) if odd_z == 0 else (odd_ref, even_ref)
            for side, ref in enumerate((low, high)):
                for p in range(HALO):
                    ls_row = (p + 1 - side) * size_z
                    div_row = (DEEP + p) * size_z
                    up, down = pair(
                        first_rows,
                        ref[ls_row : ls_row + TILE],
                        ref[ls_row + size_z - TILE : ls_row + size_z],
                        ref[div_row : div_row + TILE],
                        ref[div_row + size_z - TILE : div_row + size_z],
                    )
                    row = (side * HALO + p) * TILE
                    up_ref[row : row + TILE] = up
                    down_ref[row : row + TILE] = down
                row = 2 * HALO * TILE + side
                up_ref[row : row + 1] = ref[flags + tiles_z - 1 : flags + tiles_z]
                down_ref[row : row + 1] = ref[flags : flags + 1]

        by_parity("gz", put_z)

    by_parity("gx", put)


class Stages:
    def __init__(self, dims, ring, open_ref, dist_ref, src_ref, gain_ref, va_ref, vb_ref, u_ref, beyond_ref):
        self.ring = ring
        self.beyond = beyond_ref
        self.size_x, self.size_z, self.size_y = dims
        self.count = self.size_y // LANES
        self.open, self.dist, self.src, self.gain = open_ref, dist_ref, src_ref, gain_ref
        self.va, self.vb, self.u = va_ref, vb_ref, u_ref
        self.wide = self.size_z + TILE
        self.tile_rows = lax.broadcasted_iota(jnp.int32, (TILE, self.size_y), 0)

    def at(self, slot):
        return jnp.bitwise_and(slot, self.ring - 1) if self.ring else slot

    def chunk(self, c):
        return slice(c * LANES, (c + 1) * LANES)

    def put(self, slot, row, levels, act):
        slot = self.at(slot)
        fluid = jnp.logical_and(levels < 0, act > 0)
        away = jnp.abs(levels)
        opened = jnp.where(fluid, 0.0, away)
        dist = jnp.where(fluid, away, 0.0)
        for c in range(self.count):
            self.open[slot, c, row : row + TILE] = opened[:, self.chunk(c)]
            self.dist[slot, c, row : row + TILE] = dist[:, self.chunk(c)]

    def put_source(self, slot, row, values):
        slot = self.at(slot)
        for c in range(self.count):
            self.src[slot, c, row : row + values.shape[0]] = values[:, self.chunk(c)]

    def put_beyond(self, slot, levels, act):
        slot = self.at(slot)
        fluid = jnp.logical_and(levels < 0, act > 0)
        opened = jnp.where(fluid, 0.0, jnp.abs(levels))
        for c in range(self.count):
            self.beyond[slot, c] = opened[:, self.chunk(c)]

    def halo_tile(self, slot, below, above, act):
        high = self.tile_rows < HALO
        self.put(slot, self.size_z, jnp.where(high, above, below), act)
        self.put_source(slot, self.size_z, pltpu.roll(jnp.where(high, below, above), HALO, 0))

    def spread(self, row):
        return jnp.broadcast_to(row, (TILE, self.size_y))

    def own_plane(self, slot, x, ls_ref, div_ref, act_ref, zl_ref, zh_ref, base, span):
        size_z = self.size_z
        tile_x = lax.div(x, TILE)
        row = (x - base) * TILE
        row = row if isinstance(x, int) else pl.multiple_of(row, TILE)
        flag, fifth = span * (TILE + 1) + tile_x - base // TILE, span * TILE + x - base
        high = self.tile_rows < HALO
        act = jnp.where(
            high, self.spread(zh_ref[pl.ds(flag, 1)]), self.spread(zl_ref[pl.ds(flag, 1)])
        )
        self.halo_tile(slot, zl_ref[pl.ds(row, TILE)], zh_ref[pl.ds(row, TILE)], act)
        levels = jnp.where(
            high, self.spread(zh_ref[pl.ds(fifth, 1)]), self.spread(zl_ref[pl.ds(fifth, 1)])
        )
        self.put_beyond(slot, levels, act)
        self.put_source(slot, 0, div_ref[x])
        for j in range(size_z // TILE):
            rows = slice(j * TILE, (j + 1) * TILE)
            self.put(slot, j * TILE, ls_ref[x, rows], self.spread(act_ref[j, pl.ds(tile_x, 1)]))

    def lateral(self, values):
        lane = lax.broadcasted_iota(jnp.int32, values[0].shape, 1)
        first, last = lane == 0, lane == LANES - 1
        left = [pltpu.roll(v, 1, 1) for v in values]
        right = [pltpu.roll(v, LANES - 1, 1) for v in values]
        lefts = [jnp.where(first, left[c - 1] if c else 0.0, left[c]) for c in range(self.count)]
        rights = [
            jnp.where(last, right[c + 1] if c + 1 < self.count else 0.0, right[c])
            for c in range(self.count)
        ]
        return lefts, rights

    def vertical(self, v):
        return pltpu.roll(v, self.wide - 1, 0), pltpu.roll(v, 1, 0)

    def near(self, ref, slot, wide):
        here, before, after = self.at(slot), self.at(slot - 1), self.at(slot + 1)
        rows = slice(0, wide)
        values = [ref[here, c] for c in range(self.count)]
        lefts, rights = self.lateral([v[:wide] for v in values])
        total = []
        for c in range(self.count):
            above, below = self.vertical(values[c])
            total.append(
                (ref[after, c, rows] + ref[before, c, rows])
                + (above[:wide] + below[:wide])
                + (lefts[c] + rights[c])
            )
        return total

    def gains(self, slot):
        ref, size_z = self.open, self.size_z
        before, after, slot = self.at(slot - 1), self.at(slot + 1), self.at(slot)
        values = [ref[slot, c] for c in range(self.count)]
        lefts, rights = self.lateral(values)
        tile_rows = self.tile_rows[:, :LANES]
        for c in range(self.count):
            dist = self.dist[slot, c]
            top = (ratio_cap - 1.0) * dist
            above, below = self.vertical(values[c])
            beyond = self.beyond[slot, c]
            above = jnp.concatenate(
                [above[:size_z], jnp.where(tile_rows == HALO - 1, beyond, above[size_z:])], 0
            )
            below = jnp.concatenate(
                [below[:size_z], jnp.where(tile_rows == HALO, beyond, below[size_z:])], 0
            )
            pieces = [
                jnp.minimum(piece, top)
                for piece in (ref[after, c], ref[before, c], above, below, lefts[c], rights[c])
            ]
            total = (pieces[0] + pieces[1]) + (pieces[2] + pieces[3]) + (pieces[4] + pieces[5])
            whole = jnp.where(dist > 0, 6.0 * dist + total, 1.0)
            gain = damping * dist / whole
            self.gain[slot, c] = gain
            self.va[slot, c] = gain * self.src[slot, c]

    def smooth_first(self, slot):
        around = self.near(self.va, slot, self.wide)
        slot = self.at(slot)
        for c in range(self.count):
            u = (2.0 * damping) * self.src[slot, c] + around[c]
            self.u[slot, c] = u
            self.vb[slot, c] = self.gain[slot, c] * u

    def image_first(self, slot):
        around = self.near(self.vb, slot, self.wide)
        slot = self.at(slot)
        for c in range(self.count):
            w = damping * self.u[slot, c] - around[c]
            self.u[slot, c] = w
            self.va[slot, c] = self.gain[slot, c] * w

    def keep_first(self, slot, x, place, div_ref, z_out, r_out, w_out, dots):
        own = slice(0, self.size_z)
        slot = self.at(slot)
        gamma, delta = [], []
        for c in range(self.count):
            ch = self.chunk(c)
            fluid = self.gain[slot, c, own] > 0
            z = self.vb[slot, c, own]
            r = jnp.where(fluid, div_ref[x, :, ch], 0.0)
            w = jnp.where(fluid, self.u[slot, c, own], 0.0)
            z_out[place + (slice(None), ch)] = z
            r_out[place + (slice(None), ch)] = r
            w_out[place + (slice(None), ch)] = w
            gamma.append(r * z)
            delta.append(z * w)
        dots[0] += self.folded(gamma)
        dots[1] += self.folded(delta)

    def smooth_second(self, slot):
        around = self.near(self.va, slot, self.wide)
        slot = self.at(slot)
        for c in range(self.count):
            u = (2.0 * damping) * self.u[slot, c] + around[c]
            self.u[slot, c] = u
            self.vb[slot, c] = self.gain[slot, c] * u

    def image_second(self, slot, place, w_ref, w_place, q_out, t_out, dots):
        own = slice(0, self.size_z)
        around = self.near(self.vb, slot, self.size_z)
        slot = self.at(slot)
        cross, last = [], []
        for c in range(self.count):
            ch = self.chunk(c)
            t = damping * self.u[slot, c, own] - around[c]
            t = jnp.where(self.gain[slot, c, own] > 0, t, 0.0)
            q = self.vb[slot, c, own]
            q_out[place + (slice(None), ch)] = q
            t_out[place + (slice(None), ch)] = t
            cross.append(w_ref[w_place + (slice(None), ch)] * q)
            last.append(q * t)
        dots[2] += self.folded(cross)
        dots[3] += self.folded(last)

    def folded(self, products):
        parts = [
            product[z0 : z0 + TILE] for product in products for z0 in range(0, self.size_z, TILE)
        ]
        while len(parts) > 1:
            parts = [sum(parts[k + 1 : k + 2], parts[k]) for k in range(0, len(parts), 2)]
        return parts[0]

    def handed(self):
        return (
            [(self.va, m) for m in range(1, 5)]
            + [(self.vb, m) for m in range(2, 6)]
            + [(self.u, m) for m in range(2, 5)]
            + [(self.gain, m) for m in range(1, 5)]
            + [(self.src, 1)]
        )


HANDED = 16


LEAD = 13
EDGE = 5


def each(first, end, stage, unroll=5):
    def body(x, carry):
        stage(x)
        return carry

    lax.fori_loop(first, end, body, 0, unroll=min(unroll, end - first))


def inner_steps(do, part, ls_ref, div_ref, act_ref, zl_ref, zh_ref, outs, dots):
    z_out, q_out, r_out, w_out, t_out = outs

    def own(x):
        do.own_plane(x, x, ls_ref, div_ref, act_ref, zl_ref, zh_ref, *part)

    def second(x):
        do.keep_first(x, x, (x,), div_ref, z_out, r_out, w_out, dots)
        do.smooth_second(x)

    def last(x):
        do.image_second(x, (x,), w_out, (x,), q_out, t_out, dots)

    def sweep(i):
        last(i - 8)
        second(i - 6)
        do.image_first(i - 4)
        do.smooth_first(i - 2)
        do.gains(i)
        own(i + 2)

    return own, second, last, sweep


def inner_first_kernel(dims, part, ls_ref, div_ref, act_ref, z_even, z_odd, *outs):
    vectors, hand_out, dots, fields = outs[:5], outs[5], outs[6], outs[7:]

    def run(odd):
        low, high = (z_odd, z_even) if odd == 0 else (z_even, z_odd)
        do = Stages(dims, RING, *fields)
        dots[...] = jnp.zeros_like(dots)
        own, second, _, sweep = inner_steps(
            do, part, ls_ref, div_ref, act_ref, low, high, vectors, dots
        )
        each(0, LEAD + 2, own)
        each(1, LEAD, do.gains)
        each(2, LEAD - 2, do.smooth_first)
        each(3, LEAD - 4, do.image_first)
        each(4, LEAD - 6, second)
        for item, (ref, m) in enumerate(do.handed()):
            hand_out[item] = ref[m]
        each(LEAD, part[1] - 2, sweep, 1)

    by_parity("gz", run)


def inner_last_kernel(
    dims, part, ls_ref, div_ref, act_ref, z_even, z_odd, w_first, dots_first, *refs
):
    held, vectors, hand_out, dots, fields = refs[:8], refs[8:13], refs[13], refs[14], refs[15:]
    size_x = dims[0]
    start, stop = part[0] - 2, size_x - 2

    def run(odd):
        low, high = (z_odd, z_even) if odd == 0 else (z_even, z_odd)
        do = Stages(dims, RING, *fields)
        dots[...] = dots_first[...]
        for ref, old, first, end in zip(
            fields, held, (-1, 0, -2, -8, -7, -9, -8, 0), (2, 2, 2, 0, 0, -2, -2, 2)
        ):
            for x in range(start + first, start + end):
                ref[x % RING] = old[x % RING]
        for x in range(start - 8, start - 6):
            vectors[3][x] = w_first[x]
        _, second, last, sweep = inner_steps(
            do, part, ls_ref, div_ref, act_ref, low, high, vectors, dots
        )
        each(start, stop, sweep, 1)
        each(stop, size_x - 1, do.gains)
        each(stop - 2, size_x - 2, do.smooth_first)
        each(stop - 4, size_x - 3, do.image_first)
        each(stop - 6, size_x - 4, second)
        each(stop - 8, size_x - 5, last)
        for item, (ref, m) in enumerate(do.handed()):
            hand_out[item] = ref[do.at(size_x - 1 - m)]

    by_parity("gz", run)


SPAN = 12


def ends_kernel(
    dims, parts, ls_ref, div_ref, act_ref, z_first_even, z_first_odd, z_last_even, z_last_odd, x_even, x_odd, c_even, c_odd,
    hand_low, hand_high, w_low, w_high, inner_dots, z_out, q_out, r_out, w_out, t_out, sums_out, dots, *fields,
):
    size_x, size_z, _ = dims
    z_first, z_last = (z_first_even, z_first_odd), (z_last_even, z_last_odd)
    do = Stages(dims, 0, *fields)
    dots[...] = inner_dots[...]

    def slot(side, m):
        return side * SPAN + m + DEEP

    def x_of(side, m):
        return m if side == 0 else size_x - 1 - m

    for side in range(2):
        for item, (ref, m) in enumerate(do.handed()):
            ref[slot(side, m)] = (hand_low, hand_high)[side][item]
        blank = jnp.zeros((TILE, LANES), f32)
        for c in range(do.count):
            do.open[slot(side, -DEEP), c, size_z : size_z + TILE] = blank
            for m in range(-HALO, 0):
                do.beyond[slot(side, m), c] = blank

    def fill_z(odd):
        cl_ref, ch_ref = (c_odd, c_even) if odd == 0 else (c_even, c_odd)
        for side in range(2):
            z_even, z_odd = (z_first, z_last)[side]
            zl_ref, zh_ref = (z_odd, z_even) if odd == 0 else (z_even, z_odd)
            for m in range(2):
                do.own_plane(
                    slot(side, m), x_of(side, m), ls_ref, div_ref, act_ref, zl_ref, zh_ref, *parts[side]
                )
            flag = 2 * HALO * TILE + side
            for p in range(HALO):
                here = slot(side, p - HALO if side == 0 else -1 - p)
                row = (side * HALO + p) * TILE
                act = jnp.where(
                    do.tile_rows < HALO,
                    do.spread(ch_ref[flag : flag + 1]),
                    do.spread(cl_ref[flag : flag + 1]),
                )
                do.halo_tile(here, cl_ref[row : row + TILE], ch_ref[row : row + TILE], act)

    def fill_x(odd):
        for side, ref in enumerate((x_odd, x_even) if odd == 0 else (x_even, x_odd)):
            flags = (DEEP + HALO) * size_z
            for p in range(DEEP):
                here = slot(side, p - DEEP if side == 0 else -1 - p)
                for j in range(size_z // TILE):
                    row = p * size_z + j * TILE
                    act = do.spread(ref[flags + j : flags + j + 1])
                    do.put(here, j * TILE, ref[row : row + TILE], act)
            for p in range(HALO):
                row = (DEEP + p) * size_z
                here = slot(side, p - HALO if side == 0 else -1 - p)
                do.put_source(here, 0, ref[row : row + size_z])

    by_parity("gz", fill_z)
    by_parity("gx", fill_x)

    def both(first, end, stage):
        def body(n, carry):
            for side in range(2):
                stage(side, side * SPAN + n, n - DEEP)
            return carry

        lax.fori_loop(first + DEEP, end + DEEP, body, 0, unroll=5)

    both(-4, 1, lambda side, here, m: do.gains(here))
    both(-3, 2, lambda side, here, m: do.smooth_first(here))
    both(-2, 3, lambda side, here, m: do.image_first(here))
    both(
        0, EDGE - 1,
        lambda side, here, m: do.keep_first(
            here, x_of(side, m), (side, m), div_ref, z_out, r_out, w_out, dots
        ),
    )
    for side in range(2):
        w_out[side, EDGE - 1] = (w_low, w_high)[side][x_of(side, EDGE - 1)]
    both(-1, 4, lambda side, here, m: do.smooth_second(here))
    both(
        0, EDGE,
        lambda side, here, m: do.image_second(
            here, (side, m), w_out, (side, m), q_out, t_out, dots
        ),
    )
    lane = lax.broadcasted_iota(jnp.int32, (1, LANES), 1)
    line = jnp.zeros((1, LANES), f32)
    for place in range(4):
        line = jnp.where(lane == place, jnp.sum(dots[place]), line)
    sums_out[...] = jnp.broadcast_to(line, sums_out.shape)


def final_kernel(
    planes, meet, sums_ref, *refs
):
    first, final, ends = refs[:5], refs[5:10], refs[10:15]
    pressure_out, residual_out, pressure, residual, sems = refs[15:]
    totals = jnp.sum(sums_ref[...], axis=0, keepdims=True)
    lane = lax.broadcasted_iota(jnp.int32, totals.shape, 1)
    gamma, delta, cross, last = [
        jnp.sum(jnp.where(lane == place, totals, 0.0), axis=1, keepdims=True) for place in range(4)
    ]
    alpha = gamma / delta
    gamma_next = gamma - 2.0 * alpha * delta + alpha * alpha * cross
    beta = gamma_next / gamma
    delta_next = delta - 2.0 * alpha * cross + alpha * alpha * last
    alpha_next = gamma_next / (delta_next - beta * gamma_next / alpha)
    size_x, _, size_y = pressure.shape
    on_first = jnp.broadcast_to(alpha + alpha_next * (1.0 + beta), (1, LANES))
    on_second = jnp.broadcast_to(-alpha_next * alpha, (1, LANES))
    on_first = jnp.concatenate([on_first] * (size_y // LANES), 1)
    on_second = jnp.concatenate([on_second] * (size_y // LANES), 1)

    def put(x, z, q, r, w, t):
        pressure[x] = on_first * z + on_second * q
        residual[x] = r - on_first * w - on_second * t

    late = (0, 2, 0, 0, 2)

    def one(x):
        edge = min(x, size_x - 1 - x)
        side = int(x >= size_x // 2)
        picked = []
        for k in range(5):
            if edge < (EDGE if late[k] else EDGE - 1):
                picked.append(ends[k][side, edge])
            else:
                picked.append((first if x < meet - late[k] else final)[k][x])
        put(x, *picked)

    for x in (*range(EDGE), meet - 2, meet - 1, *range(size_x - EDGE, size_x)):
        one(x)

    def from_first(x, carry):
        put(x, *(ref[x] for ref in first))
        return carry

    def from_final(x, carry):
        put(x, *(ref[x] for ref in final))
        return carry

    copies = []
    for chunk in range(size_x // planes):
        begin, end = chunk * planes, (chunk + 1) * planes
        for low, high, step in ((EDGE, meet - 2, from_first), (meet, size_x - EDGE, from_final)):
            low, high = max(begin, low), min(end, high)
            if low < high:
                lax.fori_loop(low, high, step, 0, unroll=min(4, high - low))
        where = pl.ds(begin, planes)
        for place, (src, dst) in enumerate(((pressure, pressure_out), (residual, residual_out))):
            copy = pltpu.make_async_copy(src.at[where], dst.at[where], sems.at[2 * chunk + place])
            copy.start()
            copies.append(copy)
    for copy in copies:
        copy.wait()


def exchange(values, axis, odd):
    count = lax.axis_size(axis)
    pairs = [(i, ((i - odd) ^ 1) + odd) for i in range(count)]
    return lax.ppermute(values, axis, [(i, j) for i, j in pairs if 0 <= j < count])


def on_device(divergence, level_set, tile_ids):
    dims = divergence.shape
    size_x, size_z, size_y = dims
    tiles_x, tiles_z = size_x // TILE, size_z // TILE
    count_x, count_z = lax.axis_size("gx"), lax.axis_size("gz")

    half = tiles_x // 2 * TILE
    parts = ((0, half), (half, size_x - half))
    z_rows = [span * TILE + span + -(-span // TILE // TILE) * TILE for _, span in parts]
    x_rows = (DEEP + HALO) * size_z + TILE
    c_rows = 2 * HALO * TILE + TILE
    x_even, x_odd, act = pl.pallas_call(
        functools.partial(pack_x_kernel, dims),
        out_shape=(array(x_rows, size_y),) * 2 + (array(tiles_z, tiles_x, size_y),),
        in_specs=[HBM_SPEC] * 3,
        out_specs=(VMEM_SPEC,) * 3,
        scratch_shapes=[
            pltpu.VMEM(tile_ids.shape, jnp.int32),
            pltpu.VMEM((2 * (DEEP + HALO), size_z, size_y), f32),
            pltpu.SemaphoreType.DMA((5,)),
        ],
        compiler_params=limit(57),
        name="pack_x",
    )(tile_ids, level_set, divergence)
    x_even = exchange(x_even, "gx", 0)
    x_odd = exchange(x_odd, "gx", 1)
    sent = pl.pallas_call(
        functools.partial(pack_z_kernel, dims, parts),
        out_shape=[array(rows, size_y) for rows in z_rows for _ in range(2)],
        in_specs=[VMEM_SPEC] * 3,
        out_specs=[VMEM_SPEC] * 4,
        compiler_params=limit(8),
        name="pack_z",
    )(level_set, divergence, act)
    z_first, z_last = [
        (exchange(sent[2 * part], "gz", 0), exchange(sent[2 * part + 1], "gz", 1))
        for part in range(2)
    ]

    def fields(planes):
        field = pltpu.VMEM((planes, size_y // LANES, size_z + ROWS, LANES), f32)
        return [field] * 7 + [pltpu.VMEM((planes, size_y // LANES, TILE, LANES), f32)]

    block = array(*dims)
    chunks, rows = size_y // LANES, size_z + ROWS
    hand = array(HANDED, chunks, rows, LANES)
    dots = array(4, TILE, LANES)
    ring = [array(RING, chunks, rows, LANES)] * 7 + [array(RING, chunks, TILE, LANES)]
    early = array(half, size_z, size_y)
    first_call = pl.pallas_call(
        functools.partial(inner_first_kernel, dims, parts[0]),
        out_shape=[early] * 5 + [hand, dots] + ring,
        in_specs=[VMEM_SPEC] * 5,
        out_specs=[VMEM_SPEC] * 15,
        compiler_params=limit(4),
        name="inner_first",
    )
    *first, hand_low, dots_first = (outs := first_call(level_set, divergence, act, *z_first))[:7]
    held = outs[7:]
    c_even, c_odd = pl.pallas_call(
        functools.partial(pack_corner_kernel, dims),
        out_shape=(array(c_rows, size_y),) * 2,
        in_specs=[VMEM_SPEC] * 3,
        out_specs=(VMEM_SPEC,) * 2,
        compiler_params=limit(8),
        name="pack_corner",
    )(x_even, x_odd, dots_first)
    c_odd = exchange(c_odd, "gz", 1)
    c_even = exchange(c_even, "gz", 0)

    last_call = pl.pallas_call(
        functools.partial(inner_last_kernel, dims, parts[1]),
        out_shape=[block] * 5 + [hand, dots],
        in_specs=[VMEM_SPEC] * 15,
        out_specs=[VMEM_SPEC] * 7,
        scratch_shapes=fields(RING),
        compiler_params=limit(12),
        name="inner_last",
    )
    *second, hand_high, dots_last = last_call(
        level_set, divergence, act, *z_last, first[3], dots_first, *held
    )

    devices = count_x * count_z
    end = array(2, EDGE, size_z, size_y)
    *ends, sums = pl.pallas_call(
        functools.partial(ends_kernel, dims, parts),
        out_shape=(end,) * 5 + (array(devices, LANES),),
        in_specs=[VMEM_SPEC] * 16,
        out_specs=(VMEM_SPEC,) * 6,
        scratch_shapes=[pltpu.VMEM((4, TILE, LANES), f32)] + fields(2 * SPAN),
        compiler_params=limit(20),
        name="ends",
    )(
        level_set, divergence, act, *z_first, *z_last, x_even, x_odd, c_even, c_odd,
        hand_low, hand_high, first[3], second[3], dots_last,
    )

    gathered = lax.all_to_all(sums, ("gx", "gz"), 0, 0, tiled=True)
    planes = TILE
    return tuple(
        pl.pallas_call(
            functools.partial(final_kernel, planes, half - 8),
            out_shape=(block,) * 2,
            in_specs=[VMEM_SPEC] * 16,
            out_specs=(HBM_SPEC,) * 2,
            scratch_shapes=[
                pltpu.VMEM(dims, f32),
                pltpu.VMEM(dims, f32),
                pltpu.SemaphoreType.DMA((2 * size_x // planes,)),
            ],
            compiler_params=limit(8),
            name="outputs",
        )(gathered, *first, *second, *ends)
    )


def solution(mesh):
    placed = (P("gx", "gz", None), P("gx", "gz", None), P("gx", "gz"))
    return jax.shard_map(
        on_device,
        mesh=mesh,
        in_specs=placed,
        out_specs=(P("gx", "gz", None), P("gx", "gz", None)),
        check_vma=False,
    )
```
